256 devices in a mesh: parts: 4 (over x, y), seq: 64 (over z, core).
Axes of the slice: x: 2, y: 2, z: 32, core: 2. Of those that a mesh axis runs over, the one named last changes fastest.
The devices are a block of a 4x8x32 slice.
Arguments:
- latent: float32 [24576, 64], P(('parts', 'seq')), parts along dimension 0, may hold values from -6 to 6
- main_hidden: bfloat16 [24576, 5120], P(('parts', 'seq')), parts along dimension 0, may hold values from -10 to 10
- main_query: bfloat16 [24576, 5120], P(('parts', 'seq')), parts along dimension 0, may hold values from -40 to 40
- text_key: bfloat16 [2048, 5120], P(('parts', 'seq')), parts along dimension 0, may hold values from -40 to 40
- text_value: bfloat16 [2048, 5120], P(('parts', 'seq')), parts along dimension 0, may hold values from -12 to 12
- text_len: int32 [4], P('parts'), parts along dimension 0, may hold values from 128 to 512
- guide_hidden: bfloat16 [24576, 1536], P(('parts', 'seq')), parts along dimension 0, may hold values from -10 to 10
- guide_query: bfloat16 [24576, 768], P(('parts', 'seq')), parts along dimension 0, may hold values from -40 to 40
- guide_key: bfloat16 [24576, 768], P(('parts', 'seq')), parts along dimension 0, may hold values from -40 to 40
- guide_value: bfloat16 [24576, 768], P(('parts', 'seq')), parts along dimension 0, may hold values from -48 to 48
- guide_out: bfloat16 [768, 1536], replicated, may hold values from -0.21875 to 0.21875
- main_head: bfloat16 [5120, 64], replicated, may hold values from -0.078125 to 0.078125
- guide_head: bfloat16 [1536, 64], replicated, may hold values from -0.15625 to 0.15625
- main_modulation: float32 [8, 5120], P('parts'), parts along dimension 0, may hold values from -1.5 to 1.5
- guide_modulation: float32 [8, 1536], P('parts'), parts along dimension 0, may hold values from -1.5 to 1.5
- guidance_scale: float32 [4], P('parts'), parts along dimension 0, may hold values from 1.5 to 3.5
- sigma_table: float32 [51], replicated, may hold values from 0 to 1, as said below
- step_index: int32 [4], P('parts'), parts along dimension 0, may hold values from 0 to 49
Outputs:
- velocity: float32 [24576, 64], P(('parts', 'seq')), parts along dimension 0
- next_latent: float32 [24576, 64], P(('parts', 'seq')), parts along dimension 0
The draws below stay inside these ranges and needn't reach their ends.
There are 4 independent parts, one for each index of `parts`. The reference program is written for one: setup_inputs(seed, part) draws one part's arguments, and reference() takes and returns one part's arrays. A program takes and returns all parts, laid end to end along the dimension named above; an argument that names none is the same for every part. Nothing has to cross between parts.
Inputs may be any that keep to these rules, and one draw needn't show every extreme that they name: `sigma_table`: falls from 1 at index 0 to a small positive value at index 50.
All inputs are finite; a program needn't handle non-finite values.
Results may differ from the reference program's by a relative error of at most 0.0055.
Values may be sent and summed in bfloat16 or wider, within the bound.
No kernel may reach another device: no remote copies, remote signals or barrier semaphores. Data moves between devices by JAX's collectives and lax.ppermute only.
A program may use at most 192 MiB of HBM per device.

```python
import math
import jax
import jax.numpy as jnp
from jax import lax

HDIM = 128
HM = 40
D = 5120
GH = 6
GA = 768
G = 1536
C = 64
TEXT = 512
STEPS = 50
TOKENS = 6144


def query_and_keys(key, query_rows, key_rows, heads):
    keys = jnp.clip(jax.random.normal(jax.random.fold_in(key, 11), (key_rows, heads * HDIM), jnp.float32), -5.0, 5.0)
    queries = 1.5 * jnp.clip(jax.random.normal(jax.random.fold_in(key, 12), (query_rows, heads * HDIM), jnp.float32), -5.0, 5.0)
    return (queries, keys)


def draw_main_query(key, part):
    return query_and_keys(jax.random.fold_in(key, 101), TOKENS, TEXT, HM)[0].astype(jnp.bfloat16)


def draw_text_key(key, part):
    return query_and_keys(jax.random.fold_in(key, 101), TOKENS, TEXT, HM)[1].astype(jnp.bfloat16)


def draw_guide_query(key, part):
    return query_and_keys(jax.random.fold_in(key, 202), TOKENS, TOKENS, GH)[0].astype(jnp.bfloat16)


def draw_guide_key(key, part):
    return query_and_keys(jax.random.fold_in(key, 202), TOKENS, TOKENS, GH)[1].astype(jnp.bfloat16)


def stream_draw(key, width, plain_scale):
    base = jnp.clip(jax.random.normal(jax.random.fold_in(key, 1), (TOKENS, width), jnp.float32), -6.0, 6.0)
    return plain_scale * base


def draw_main_hidden(key, part):
    return stream_draw(jax.random.fold_in(key, 303), D, 0.5).astype(jnp.bfloat16)


def draw_guide_hidden(key, part):
    return stream_draw(jax.random.fold_in(key, 404), G, 0.3).astype(jnp.bfloat16)


def draw_sigma_table(key, part):
    increments = jnp.exp(jax.random.uniform(jax.random.fold_in(key, 505), (STEPS,), jnp.float32, math.log(0.2), math.log(6.0)))
    climbed = jnp.concatenate([jnp.zeros((1,), jnp.float32), jnp.cumsum(increments)])
    return 1.0 - 0.97 * climbed / climbed[-1]


def block_levels(stream_key, shape, pieces, least, high):
    level = 1.0
    for dim, parts in pieces:
        heights = jax.random.uniform(jax.random.fold_in(jax.random.fold_in(stream_key, 6), dim), (parts,), jnp.float32, least / len(pieces), high / len(pieces))
        level = level * jnp.repeat(jnp.exp(heights), shape[dim] // parts).reshape((-1,) + (1,) * (len(shape) - 1 - dim))
    return level


def centred(stream_key, dims, scale, most, cuts=(), kind=jnp.bfloat16):
    gain = block_levels(stream_key, dims, cuts, -0.22, 0.18) if cuts else 1.0
    values = jax.random.normal(stream_key, dims, jnp.float32) * scale * gain
    return jnp.minimum(jnp.maximum(values, -most), most).astype(kind)


def setup_inputs(seed: int = 0, part: int = 0) -> dict:
    arg_keys = jax.random.split(jax.random.key(seed), 19)
    part_splits = jax.random.split(jax.random.fold_in(arg_keys[18], part), 19)
    latent = centred(part_splits[0], (TOKENS, C), 1.0, 6.0, ((0, 64),), jnp.float32)
    main_hidden = draw_main_hidden(jax.random.fold_in(jax.random.fold_in(arg_keys[18], part), 71), part)
    main_query = draw_main_query(jax.random.fold_in(jax.random.fold_in(arg_keys[18], part), 71), part)
    text_key = draw_text_key(jax.random.fold_in(jax.random.fold_in(arg_keys[18], part), 71), part)
    text_value = centred(part_splits[4], (TEXT, D), 2.0, 12.0, ((0, 64),))
    text_len = jax.random.randint(part_splits[5], (1,), TEXT // 4, TEXT + 1).astype(jnp.int32)
    guide_hidden = draw_guide_hidden(jax.random.fold_in(jax.random.fold_in(arg_keys[18], part), 71), part)
    guide_query = draw_guide_query(jax.random.fold_in(jax.random.fold_in(arg_keys[18], part), 71), part)
    guide_key = draw_guide_key(jax.random.fold_in(jax.random.fold_in(arg_keys[18], part), 71), part)
    guide_value = centred(part_splits[9], (TOKENS, GA), 8.0, 48.0, ((0, 64),))
    guide_out = centred(arg_keys[10], (GA, G), GA ** -0.5, 0.21875)
    main_head = centred(arg_keys[11], (D, C), D ** -0.5, 0.078125)
    guide_head = centred(arg_keys[12], (G, C), G ** -0.5, 0.15625)
    main_modulation = centred(part_splits[13], (2, D), 0.3, 1.5, (), jnp.float32)
    guide_modulation = centred(part_splits[14], (2, G), 0.3, 1.5, (), jnp.float32)
    guidance_scale = jnp.clip(jax.random.uniform(part_splits[15], (1,), jnp.float32, 1.5, 3.5), 1.5, 3.5)
    sigma_table = draw_sigma_table(jax.random.fold_in(arg_keys[18], 71), part)
    step_index = jax.random.randint(part_splits[17], (1,), 0, STEPS).astype(jnp.int32)
    return dict(latent=latent, main_hidden=main_hidden, main_query=main_query, text_key=text_key, text_value=text_value, text_len=text_len, guide_hidden=guide_hidden, guide_query=guide_query, guide_key=guide_key, guide_value=guide_value, guide_out=guide_out, main_head=main_head, guide_head=guide_head, main_modulation=main_modulation, guide_modulation=guide_modulation, guidance_scale=guidance_scale, sigma_table=sigma_table, step_index=step_index)


def start_state(height, heads, head_size):
    return (jnp.full((heads, height), -1e+30, jnp.float32), jnp.zeros((heads, height), jnp.float32), jnp.zeros((heads, height, head_size), jnp.float32))

def fold_step(running, queries, keys, values, heads, valid):
    height = queries.shape[0]
    head_size = queries.shape[1] // heads
    query_heads = queries.reshape(height, heads, head_size).astype(jnp.float32)
    key_heads = keys.reshape(keys.shape[0], heads, head_size).astype(jnp.float32)
    value_heads = values.reshape(values.shape[0], heads, head_size).astype(jnp.float32)
    scores = jnp.einsum('qhd,khd->hqk', query_heads, key_heads) * head_size ** (-0.5)
    scores = jnp.where(valid[None, None, :], scores, -1e+30)
    peak_old, totals, accumulated = running
    peak_new = jnp.maximum(peak_old, lax.optimization_barrier(jnp.max(scores, axis=-1)))
    weights = jnp.where(valid[None, None, :], jnp.exp(scores - peak_new[..., None]), 0.0)
    factor = jnp.exp(peak_old - peak_new)
    totals = totals * factor + lax.optimization_barrier(jnp.sum(weights, axis=-1))
    rounded = weights.astype(jnp.bfloat16).astype(jnp.float32)
    accumulated = accumulated * factor[..., None] + jnp.einsum('hqk,khd->hqd', rounded, value_heads)
    return (peak_new, totals, accumulated)

def finish(running):
    peak, totals, accumulated = running
    result = accumulated / totals[..., None]
    return result.transpose(1, 0, 2).reshape(result.shape[1], -1).astype(jnp.bfloat16)

def attention(queries, keys, values, heads, valid):
    height = queries.shape[0]
    block = math.gcd(height, 512)
    head_size = queries.shape[1] // heads
    blocks = queries.reshape(height // block, block, queries.shape[1])

    def one_block(query_block):
        state = start_state(block, heads, head_size)
        return finish(fold_step(state, query_block, keys, values, heads, valid))
    return lax.map(one_block, blocks).reshape(height, -1)

def head_out(summed, modulation, head_weight):
    centered = summed - lax.optimization_barrier(jnp.mean(summed, axis=-1, keepdims=True))
    spread = lax.optimization_barrier(jnp.mean(centered * centered, axis=-1, keepdims=True))
    normed = centered * lax.rsqrt(spread + 1e-06)
    shaped = (normed * (1.0 + modulation[1]) + modulation[0]).astype(jnp.bfloat16)
    return jnp.dot(shaped, head_weight, preferred_element_type=jnp.float32)

def reference(latent, main_hidden, main_query, text_key, text_value, text_len, guide_hidden, guide_query, guide_key, guide_value, guide_out, main_head, guide_head, main_modulation, guide_modulation, guidance_scale, sigma_table, step_index):
    live = jnp.arange(text_key.shape[0], dtype=jnp.int32) < text_len[0]
    main_attended = attention(main_query, text_key, text_value, HM, live)
    every = jnp.ones((guide_key.shape[0],), dtype=bool)
    guide_attended = attention(guide_query, guide_key, guide_value, GH, every)
    main_sum = main_hidden.astype(jnp.float32) + main_attended.astype(jnp.float32)
    guide_sum = guide_hidden.astype(jnp.float32) + jnp.dot(guide_attended, guide_out, preferred_element_type=jnp.float32)
    main_velocity = head_out(main_sum, main_modulation, main_head)
    guide_velocity = head_out(guide_sum, guide_modulation, guide_head)
    velocity = guide_velocity + guidance_scale[0] * (main_velocity - guide_velocity)
    positions = jnp.arange(sigma_table.shape[0], dtype=jnp.int32)
    sigma_now = jnp.sum(jnp.where(positions == step_index[0], sigma_table, 0.0))
    sigma_next = jnp.sum(jnp.where(positions == step_index[0] + 1, sigma_table, 0.0))
    next_latent = latent + (sigma_next - sigma_now) * velocity
    return (velocity, next_latent)
```

```python
import functools

import jax
import jax.numpy as jnp
from jax import lax
from jax.experimental import pallas as pl
from jax.experimental.pallas import tpu as pltpu
from jax.sharding import PartitionSpec as P

HDIM = 128
LOW = -1e30
LOG2E = 1.4426950408889634
TEXT_TURNS = 4
TEXT_PIECES = 4


def contract(a, b, b_dim):
    return lax.dot_general(
        a, b, (((1,), (b_dim,)), ((), ())), preferred_element_type=jnp.float32
    )


def attend(heads, pieces, start, per_chunk, chunks, masked, first, last, *refs):
    at = 0
    if masked:
        live = refs[0][...] > 0.0
        at = 1
    q_refs, at = refs[at : at + 2], at + 2
    chunk_refs, at = refs[at : at + chunks * per_chunk], at + chunks * per_chunk
    if not first:
        states, at = refs[at : at + 2 * pieces], at + 2 * pieces
    outs = refs[at:]
    rate = HDIM ** (-0.5) * LOG2E
    width = q_refs[0].shape[1]
    rows = q_refs[0].shape[0]
    count = heads // pieces
    for i in range(heads):
        piece, own = i // count, i % count
        at_q = slice((start + i) * HDIM, (start + i + 1) * HDIM)
        at_v = slice(width + (start + i) * HDIM, width + (start + i + 1) * HDIM)
        at_acc = slice(own * HDIM, (own + 1) * HDIM)
        at_out = slice(i * HDIM, (i + 1) * HDIM)
        q = jnp.concatenate([r[:, at_q] for r in q_refs], axis=0)
        k = jnp.concatenate([r[:, at_q] for r in chunk_refs], axis=0)
        v = jnp.concatenate([r[:, at_v] for r in chunk_refs], axis=0)
        scores = contract(q, k, 1)
        if masked:
            scores = jnp.where(live, scores, LOW)
        peak = jnp.max(scores, axis=-1, keepdims=True)
        if not first:
            acc_in, ml_in = states[2 * piece : 2 * piece + 2]
            peak_old = ml_in[:, own : own + 1]
            peak = jnp.maximum(peak, peak_old)
        weights = jnp.exp2((scores - peak) * rate)
        if masked:
            weights = jnp.where(live, weights, 0.0)
        total = jnp.sum(weights, axis=-1, keepdims=True)
        acc = contract(weights.astype(jnp.bfloat16), v, 0)
        if not first:
            factor = jnp.exp2((peak_old - peak) * rate)
            total = total + ml_in[:, 64 + own : 65 + own] * factor
            acc = acc + acc_in[:, at_acc] * factor
        if last:
            acc = (acc / total).astype(jnp.bfloat16)
            outs[0][:, at_out] = acc[:rows]
            outs[1][:, at_out] = acc[rows:]
        else:
            outs[0][:, at_out] = acc
            outs[1][:, own : own + 1] = peak
            outs[1][:, 64 + own : 65 + own] = total


def attend_group(start, heads, per_chunk, queries, chunks, live, states, last, name):
    rows = queries[0].shape[0]
    width = heads * HDIM
    keys = sum(c.shape[0] for c in chunks)
    pieces = max(1, len(states))
    operands = ([live] if live is not None else []) + list(queries) + list(chunks)
    operands += [x for pair in states for x in pair]
    if last:
        shapes = [jax.ShapeDtypeStruct((rows, width), jnp.bfloat16)] * 2
    else:
        shapes = [
            jax.ShapeDtypeStruct((2 * rows, width), jnp.float32),
            jax.ShapeDtypeStruct((2 * rows, HDIM), jnp.float32),
        ]
    spec = pl.BlockSpec(memory_space=pltpu.VMEM)
    return pl.pallas_call(
        functools.partial(
            attend, heads, pieces, start, per_chunk, len(chunks) // per_chunk,
            live is not None, not states, last,
        ),
        out_shape=shapes,
        in_specs=[spec] * len(operands),
        out_specs=[spec] * 2,
        cost_estimate=pl.CostEstimate(
            flops=8 * rows * keys * width,
            transcendentals=2 * rows * keys * heads,
            bytes_accessed=sum(o.size * o.dtype.itemsize for o in operands),
        ),
        compiler_params=pltpu.CompilerParams(vmem_limit_bytes=16 * 2**20),
        name=name,
    )(*operands)


def head_out(summed, modulation, head_weight):
    centered = summed - jnp.mean(summed, axis=-1, keepdims=True)
    spread = jnp.mean(centered * centered, axis=-1, keepdims=True)
    normed = centered * lax.rsqrt(spread + 1e-06)
    shaped = (normed * (1.0 + modulation[1]) + modulation[0]).astype(jnp.bfloat16)
    return jnp.dot(shaped, head_weight, preferred_element_type=jnp.float32)


def per_device(
    members,
    latent,
    main_hidden,
    main_query,
    text_key,
    text_value,
    text_len,
    guide_hidden,
    guide_query,
    guide_key,
    guide_value,
    guide_out,
    main_head,
    guide_head,
    main_modulation,
    guide_modulation,
    guidance_scale,
    sigma_table,
    step_index,
):
    ring = members // 2
    me = lax.axis_index("seq")
    core, place = lax.rem(me, 2), lax.div(me, 2)
    partner = [(i, i ^ 1) for i in range(members)]
    ahead = [(i, (i + 2) % members) for i in range(members)]
    behind = [(i, (i - 2) % members) for i in range(members)]

    def half(x, which):
        width = x.shape[1] // 2
        return lax.dynamic_slice_in_dim(x, which * width, width, axis=1)

    def swap(x):
        return lax.ppermute(x, "seq", partner)

    def pair(k, v, which):
        return jnp.concatenate([half(k, which), half(v, which)], axis=1)

    text_other = swap(pair(text_key, text_value, 1 - core))
    guide_other = swap(pair(guide_key, guide_value, 1 - core))
    guide_own = pair(guide_key, guide_value, core)
    text_both = jnp.concatenate([pair(text_key, text_value, core), text_other], axis=0)
    main_queries = (half(main_query, core), swap(half(main_query, 1 - core)))
    guide_queries = (half(guide_query, core), swap(half(guide_query, 1 - core)))

    rows = text_key.shape[0]
    inner = jnp.arange(2 * rows, dtype=jnp.int32)
    inner = jnp.where(inner < rows, core * rows + inner, (1 - core) * rows + inner - rows)
    main_heads = main_head.shape[0] // HDIM // 2
    guide_heads = guide_out.shape[0] // HDIM // 2
    order = [0] + [j for s in range(1, ring // 2) for j in (s, ring - s)] + [ring // 2]
    text_turn = ring // TEXT_TURNS
    turns = [order[i : i + text_turn] for i in range(0, ring, text_turn)]
    pairs = [order[i : i + 2] for i in range(0, ring, 2)]
    piece_heads = main_heads // TEXT_PIECES

    def live_keys(group):
        owner = lax.rem(place - jnp.array(group, dtype=jnp.int32) + ring, ring)
        position = (owner[:, None] * (2 * rows) + inner[None, :]).reshape(1, -1)
        return (position < text_len[0]).astype(jnp.float32)

    lives = [live_keys(g) for g in turns]
    held = {}
    text_states = [[] for _ in range(TEXT_PIECES)]
    guide_state = []

    def text_piece(turn, piece):
        text_states[piece] = [
            attend_group(
                piece * piece_heads, piece_heads, 1, main_queries, [held[j][1] for j in turns[turn]],
                lives[turn], text_states[piece], False, "text_attention",
            )
        ]
        return text_states[piece][0][1]

    def text_last():
        return attend_group(
            0, main_heads, 1, main_queries, [held[j][1] for j in turns[-1]],
            lives[-1], [s[0] for s in text_states], True, "text_attention",
        )

    def guide_pair(k, state):
        chunks = [held[j][c] for j in pairs[k - 1] for c in (0, 2)]
        return attend_group(
            0, guide_heads, 2, guide_queries, chunks, None, state, k == len(pairs), "guide_attention"
        )

    def behind_of(arrays, *after):
        out = lax.optimization_barrier(tuple(arrays) + tuple(after))
        return list(out[: len(arrays)])

    up = [guide_own, text_both, guide_other]
    down = list(up)
    held[0] = tuple(up)
    before = None
    for step in range(1, ring // 2 + 1):
        both = step < ring - step
        fresh_up, fresh_down = [None] * 3, [None] * 3
        for c in range(3):
            after = []
            if step > 1:
                if c > 0:
                    after += [up[c - 1], down[c - 1]]
                elif before is not None:
                    after += before
                if c == 1 and step > 2:
                    guide_state = [guide_pair(step - 2, guide_state)]
                    after.append(guide_state[0][1])
                if c == 2:
                    turn, piece = divmod(step - 1, text_turn // 2)
                    if turn >= 1 and piece < TEXT_PIECES:
                        after.append(text_piece(turn - 1, piece))
            sent = [up[c], down[c]] if both else [up[c]]
            if after:
                sent = behind_of(sent, *after)
            fresh_up[c] = lax.ppermute(sent[0], "seq", ahead)
            if both:
                fresh_down[c] = lax.ppermute(sent[1], "seq", behind)
        before = [up[2], down[2]]
        up = fresh_up
        held[step] = tuple(up)
        if both:
            down = fresh_down
            held[ring - step] = tuple(down)

    guide_state = [guide_pair(ring // 2 - 1, guide_state)]
    main_own, main_theirs = text_last()
    guide_state = [behind_of(guide_state[0], main_own)]
    guide_state = guide_pair(ring // 2, guide_state)

    def whole(own, theirs):
        back = swap(theirs)
        return jnp.where(
            core == 0, jnp.concatenate([own, back], axis=1), jnp.concatenate([back, own], axis=1)
        )

    main_sum = main_hidden.astype(jnp.float32) + whole(main_own, main_theirs).astype(jnp.float32)
    main_velocity = head_out(main_sum, main_modulation, main_head)

    projected = jnp.dot(whole(*guide_state), guide_out, preferred_element_type=jnp.float32)
    guide_sum = guide_hidden.astype(jnp.float32) + projected
    guide_velocity = head_out(guide_sum, guide_modulation, guide_head)
    velocity = guide_velocity + guidance_scale[0] * (main_velocity - guide_velocity)
    positions = jnp.arange(sigma_table.shape[0], dtype=jnp.int32)
    sigma_now = jnp.sum(jnp.where(positions == step_index[0], sigma_table, 0.0))
    sigma_next = jnp.sum(jnp.where(positions == step_index[0] + 1, sigma_table, 0.0))
    next_latent = latent + (sigma_next - sigma_now) * velocity
    return (velocity, next_latent)


def solution(mesh):
    placed = (
        P(("parts", "seq"), None),
        P(("parts", "seq"), None),
        P(("parts", "seq"), None),
        P(("parts", "seq"), None),
        P(("parts", "seq"), None),
        P("parts"),
        P(("parts", "seq"), None),
        P(("parts", "seq"), None),
        P(("parts", "seq"), None),
        P(("parts", "seq"), None),
        P(),
        P(),
        P(),
        P("parts", None),
        P("parts", None),
        P("parts"),
        P(),
        P("parts"),
    )
    return jax.shard_map(
        functools.partial(per_device, mesh.shape["seq"]),
        mesh=mesh,
        in_specs=placed,
        out_specs=(P(("parts", "seq"), None), P(("parts", "seq"), None)),
        check_vma=False,
    )
```

```python
import functools

import jax
import jax.numpy as jnp
from jax import lax
from jax.experimental import pallas as pl
from jax.experimental.pallas import tpu as pltpu
from jax.sharding import PartitionSpec as P

HDIM = 128
LOW = -1e30
LOG2E = 1.4426950408889634
TEXT_CHAINS = 2
KEY_BLOCK = 1024


def contract(a, b, b_dim):
    return lax.dot_general(
        a, b, (((1,), (b_dim,)), ((), ())), preferred_element_type=jnp.float32
    )


def text_attend(first_head, heads, live_ref, qa_ref, qb_ref, *refs):
    chunk_refs, outs = refs[:-2], refs[-2:]
    live = live_ref[...] > 0.0
    rate = HDIM ** (-0.5) * LOG2E
    rows = qa_ref.shape[0]
    for i in range(heads):
        at_q = slice((first_head + i) * HDIM, (first_head + i + 1) * HDIM)
        at_k = slice(i * HDIM, (i + 1) * HDIM)
        at_v = slice((heads + i) * HDIM, (heads + i + 1) * HDIM)
        q = jnp.concatenate([qa_ref[:, at_q], qb_ref[:, at_q]], axis=0)
        k = jnp.concatenate([r[:, at_k] for r in chunk_refs], axis=0)
        v = jnp.concatenate([r[:, at_v] for r in chunk_refs], axis=0)
        scores = jnp.where(live, contract(q, k, 1), LOW)
        peak = jnp.max(scores, axis=-1, keepdims=True)
        weights = jnp.where(live, jnp.exp2((scores - peak) * rate), 0.0)
        total = jnp.sum(weights, axis=-1, keepdims=True)
        acc = (contract(weights.astype(jnp.bfloat16), v, 0) / total).astype(jnp.bfloat16)
        outs[0][:, at_k] = acc[:rows]
        outs[1][:, at_k] = acc[rows:]


def text_attention(first_head, heads, queries, chunks, live):
    rows = queries[0].shape[0]
    keys = sum(c.shape[0] for c in chunks)
    operands = [live, *queries, *chunks]
    spec = pl.BlockSpec(memory_space=pltpu.VMEM)
    return pl.pallas_call(
        functools.partial(text_attend, first_head, heads),
        out_shape=[jax.ShapeDtypeStruct((rows, heads * HDIM), jnp.bfloat16)] * 2,
        in_specs=[spec] * len(operands),
        out_specs=[spec] * 2,
        cost_estimate=pl.CostEstimate(
            flops=8 * rows * keys * heads * HDIM,
            transcendentals=2 * rows * keys * heads,
            bytes_accessed=sum(o.size * o.dtype.itemsize for o in operands),
        ),
        name="text_attention",
    )(*operands)


def guide_attend(heads, half_ref, qa_ref, qb_ref, k_ref, v_ref, own_ref, theirs_ref, acc, peaks, totals):
    del half_ref
    rate = HDIM ** (-0.5) * LOG2E
    rows = qa_ref.shape[0]

    @pl.when(pl.program_id(0) == 0)
    def _():
        acc[...] = jnp.zeros_like(acc)
        totals[...] = jnp.zeros_like(totals)
        peaks[...] = jnp.full_like(peaks, LOW)

    for h in range(heads):
        cols = slice(h * HDIM, (h + 1) * HDIM)
        q = jnp.concatenate([qa_ref[:, cols], qb_ref[:, cols]], axis=0)
        scores = contract(q, k_ref[:, cols], 1)
        peak_old = peaks[h]
        peak = jnp.maximum(peak_old[:, :1], jnp.max(scores, axis=-1, keepdims=True))
        weights = jnp.exp2((scores - peak) * rate)
        partial = weights[:, :HDIM]
        for j in range(1, weights.shape[1] // HDIM):
            partial = partial + weights[:, j * HDIM : (j + 1) * HDIM]
        factor = jnp.exp2((peak_old - peak) * rate)
        totals[h] = totals[h] * factor + partial
        acc[h] = acc[h] * factor + contract(weights.astype(jnp.bfloat16), v_ref[:, cols], 0)
        peaks[h] = jnp.broadcast_to(peak, peak_old.shape)

    @pl.when(pl.program_id(0) == pl.num_programs(0) - 1)
    def _():
        for h in range(heads):
            cols = slice(h * HDIM, (h + 1) * HDIM)
            total = jnp.sum(totals[h], axis=-1, keepdims=True)
            out = (acc[h] / total).astype(jnp.bfloat16)
            own_ref[:, cols] = out[:rows]
            theirs_ref[:, cols] = out[rows:]


def guide_attention(heads, half, queries, gathered):
    rows, width = queries[0].shape
    keys = gathered.shape[0]
    block = min(KEY_BLOCK, keys)
    fixed = pl.BlockSpec((rows, width), lambda i, half: (0, 0))
    state = pltpu.VMEM((heads, 2 * rows, HDIM), jnp.float32)
    return pl.pallas_call(
        functools.partial(guide_attend, heads),
        out_shape=[jax.ShapeDtypeStruct((rows, width), jnp.bfloat16)] * 2,
        grid_spec=pltpu.PrefetchScalarGridSpec(
            num_scalar_prefetch=1,
            grid=(keys // block,),
            in_specs=[
                fixed,
                fixed,
                pl.BlockSpec((block, width), lambda i, half: (i, half[0])),
                pl.BlockSpec((block, width), lambda i, half: (i, 2 + half[0])),
            ],
            out_specs=[fixed, fixed],
            scratch_shapes=[state, state, state],
        ),
        compiler_params=pltpu.CompilerParams(dimension_semantics=("arbitrary",)),
        cost_estimate=pl.CostEstimate(
            flops=8 * rows * keys * width,
            transcendentals=2 * rows * keys * heads,
            bytes_accessed=4 * keys * width,
        ),
        name="guide_attention",
    )(half, *queries, gathered, gathered)


def head_out(summed, modulation, head_weight):
    centered = summed - jnp.mean(summed, axis=-1, keepdims=True)
    spread = jnp.mean(centered * centered, axis=-1, keepdims=True)
    normed = centered * lax.rsqrt(spread + 1e-06)
    shaped = (normed * (1.0 + modulation[1]) + modulation[0]).astype(jnp.bfloat16)
    return jnp.dot(shaped, head_weight, preferred_element_type=jnp.float32)


def per_device(
    members,
    latent,
    main_hidden,
    main_query,
    text_key,
    text_value,
    text_len,
    guide_hidden,
    guide_query,
    guide_key,
    guide_value,
    guide_out,
    main_head,
    guide_head,
    main_modulation,
    guide_modulation,
    guidance_scale,
    sigma_table,
    step_index,
):
    ring = members // 2
    me = lax.axis_index("seq")
    core, place = lax.rem(me, 2), lax.div(me, 2)
    partner = [(i, i ^ 1) for i in range(members)]
    ahead = [(i, (i + 2) % members) for i in range(members)]
    behind = [(i, (i - 2) % members) for i in range(members)]

    def half(x, which):
        width = x.shape[1] // 2
        return lax.dynamic_slice_in_dim(x, which * width, width, axis=1)

    def swap(x):
        return lax.ppermute(x, "seq", partner)

    def pair(k, v, which):
        return jnp.concatenate([half(k, which), half(v, which)], axis=1)

    guide_all = lax.all_gather(
        jnp.concatenate([guide_key, guide_value], axis=1), "seq", axis=0, tiled=True
    )
    mine = jnp.concatenate([half(text_key, core), half(text_value, core)], axis=1)
    theirs = jnp.concatenate([half(text_key, 1 - core), half(text_value, 1 - core)], axis=1)
    text_both = jnp.concatenate([mine, swap(theirs)], axis=0)
    main_queries = (half(main_query, core), swap(half(main_query, 1 - core)))
    guide_queries = (half(guide_query, core), swap(half(guide_query, 1 - core)))

    main_heads = main_head.shape[0] // HDIM // 2
    guide_heads = guide_out.shape[0] // HDIM // 2
    part = text_both.shape[1] // 2 // TEXT_CHAINS
    key_width = text_both.shape[1] // 2
    chains = [
        jnp.concatenate(
            [text_both[:, c * part : (c + 1) * part], text_both[:, key_width + c * part : key_width + (c + 1) * part]],
            axis=1,
        )
        for c in range(TEXT_CHAINS)
    ]
    up, down = list(chains), list(chains)
    held = {0: chains}
    order = [0]
    for step in range(1, ring // 2 + 1):
        both = step < ring - step
        up = [lax.ppermute(x, "seq", ahead) for x in up]
        held[step] = up
        order.append(step)
        if both:
            down = [lax.ppermute(x, "seq", behind) for x in down]
            held[ring - step] = down
            order.append(ring - step)

    rows = text_key.shape[0]
    inner = jnp.arange(2 * rows, dtype=jnp.int32)
    inner = jnp.where(inner < rows, core * rows + inner, (1 - core) * rows + inner - rows)
    owner = lax.rem(place - jnp.array(order, dtype=jnp.int32) + ring, ring)
    position = (owner[:, None] * (2 * rows) + inner[None, :]).reshape(1, -1)
    live = (position < text_len[0]).astype(jnp.float32)
    per_chain = main_heads // TEXT_CHAINS
    parts = [
        text_attention(c * per_chain, per_chain, main_queries, [held[j][c] for j in order], live)
        for c in range(TEXT_CHAINS)
    ]
    main_own = jnp.concatenate([p[0] for p in parts], axis=1)
    main_theirs = jnp.concatenate([p[1] for p in parts], axis=1)

    def whole(own, theirs):
        back = swap(theirs)
        return jnp.where(
            core == 0, jnp.concatenate([own, back], axis=1), jnp.concatenate([back, own], axis=1)
        )

    main_sum = main_hidden.astype(jnp.float32) + whole(main_own, main_theirs).astype(jnp.float32)
    main_velocity = head_out(main_sum, main_modulation, main_head)

    main_velocity = lax.optimization_barrier(main_velocity)

    guide_state = guide_attention(guide_heads, core.reshape(1), guide_queries, guide_all)
    projected = jnp.dot(whole(*guide_state), guide_out, preferred_element_type=jnp.float32)
    guide_sum = guide_hidden.astype(jnp.float32) + projected
    guide_velocity = head_out(guide_sum, guide_modulation, guide_head)
    velocity = guide_velocity + guidance_scale[0] * (main_velocity - guide_velocity)
    positions = jnp.arange(sigma_table.shape[0], dtype=jnp.int32)
    sigma_now = jnp.sum(jnp.where(positions == step_index[0], sigma_table, 0.0))
    sigma_next = jnp.sum(jnp.where(positions == step_index[0] + 1, sigma_table, 0.0))
    next_latent = latent + (sigma_next - sigma_now) * velocity
    return (velocity, next_latent)


def solution(mesh):
    placed = (
        P(("parts", "seq"), None),
        P(("parts", "seq"), None),
        P(("parts", "seq"), None),
        P(("parts", "seq"), None),
        P(("parts", "seq"), None),
        P("parts"),
        P(("parts", "seq"), None),
        P(("parts", "seq"), None),
        P(("parts", "seq"), None),
        P(("parts", "seq"), None),
        P(),
        P(),
        P(),
        P("parts", None),
        P("parts", None),
        P("parts"),
        P(),
        P("parts"),
    )
    return jax.shard_map(
        functools.partial(per_device, mesh.shape["seq"]),
        mesh=mesh,
        in_specs=placed,
        out_specs=(P(("parts", "seq"), None), P(("parts", "seq"), None)),
        check_vma=False,
    )
```

```python
import functools

import jax
import jax.numpy as jnp
from jax import lax
from jax.experimental import pallas as pl
from jax.experimental.pallas import tpu as pltpu
from jax.sharding import PartitionSpec as P

HDIM = 128
LOW = -1e30
LOG2E = 1.4426950408889634
TEXT_CHAINS = 2
KEY_BLOCK = 2048


def contract(a, b, b_dim):
    return lax.dot_general(
        a, b, (((1,), (b_dim,)), ((), ())), preferred_element_type=jnp.float32
    )


def text_attend(first_head, heads, live_ref, qa_ref, qb_ref, *refs):
    chunk_refs, outs = refs[:-2], refs[-2:]
    live = live_ref[...] > 0.0
    rate = HDIM ** (-0.5) * LOG2E
    rows = qa_ref.shape[0]

    def one_head(i):
        at_q = pl.ds(pl.multiple_of((first_head + i) * HDIM, HDIM), HDIM)
        at_k = pl.ds(pl.multiple_of(i * HDIM, HDIM), HDIM)
        at_v = pl.ds(pl.multiple_of((heads + i) * HDIM, HDIM), HDIM)
        q = jnp.concatenate([qa_ref[:, at_q], qb_ref[:, at_q]], axis=0)
        k = jnp.concatenate([r[:, at_k] for r in chunk_refs], axis=0)
        v = jnp.concatenate([r[:, at_v] for r in chunk_refs], axis=0)
        scores = jnp.where(live, contract(q, k, 1), LOW)
        peak = jnp.max(scores, axis=-1, keepdims=True)
        weights = jnp.where(live, jnp.exp2((scores - peak) * rate), 0.0)
        total = jnp.sum(weights, axis=-1, keepdims=True)
        acc = (contract(weights.astype(jnp.bfloat16), v, 0) / total).astype(jnp.bfloat16)
        outs[0][:, at_k] = acc[:rows]
        outs[1][:, at_k] = acc[rows:]

    @pl.loop(0, heads // 2)
    def _(i):
        one_head(2 * i)
        one_head(2 * i + 1)


def text_attention(first_head, heads, queries, chunks, live):
    rows = queries[0].shape[0]
    keys = sum(c.shape[0] for c in chunks)
    operands = [live, *queries, *chunks]
    spec = pl.BlockSpec(memory_space=pltpu.VMEM)
    return pl.pallas_call(
        functools.partial(text_attend, first_head, heads),
        out_shape=[jax.ShapeDtypeStruct((rows, heads * HDIM), jnp.bfloat16)] * 2,
        in_specs=[spec] * len(operands),
        out_specs=[spec] * 2,
        cost_estimate=pl.CostEstimate(
            flops=8 * rows * keys * heads * HDIM,
            transcendentals=2 * rows * keys * heads,
            bytes_accessed=sum(o.size * o.dtype.itemsize for o in operands),
        ),
        name="text_attention",
    )(*operands)


def guide_attend(heads, half_ref, qa_ref, qb_ref, k_ref, v_ref, own_ref, theirs_ref, acc, peaks, totals):
    del half_ref
    rate = HDIM ** (-0.5) * LOG2E
    rows = qa_ref.shape[0]

    @pl.when(pl.program_id(0) == 0)
    def _():
        acc[...] = jnp.zeros_like(acc)
        totals[...] = jnp.zeros_like(totals)
        peaks[...] = jnp.full_like(peaks, LOW)

    blocks = [slice(h * HDIM, (h + 1) * HDIM) for h in range(heads)]
    scores, tops, weights = [], [], []
    for cols in blocks:
        q = jnp.concatenate([qa_ref[:, cols], qb_ref[:, cols]], axis=0)
        scores.append(contract(q, k_ref[:, cols], 1))
    for h in range(heads):
        top = jnp.max(scores[h], axis=-1, keepdims=True)
        tops.append(jnp.maximum(peaks[h], top))
    for h in range(heads):
        weights.append(jnp.exp2((scores[h] - tops[h][:, :1]) * rate))
    for h, cols in enumerate(blocks):
        partial = weights[h][:, :HDIM]
        for j in range(1, weights[h].shape[1] // HDIM):
            partial = partial + weights[h][:, j * HDIM : (j + 1) * HDIM]
        fresh = contract(weights[h].astype(jnp.bfloat16), v_ref[:, cols], 0)
        factor = jnp.exp2((peaks[h] - tops[h]) * rate)
        totals[h] = totals[h] * factor + partial
        acc[h] = acc[h] * factor + fresh
        peaks[h] = tops[h]

    @pl.when(pl.program_id(0) == pl.num_programs(0) - 1)
    def _():
        for h in range(heads):
            cols = slice(h * HDIM, (h + 1) * HDIM)
            total = jnp.sum(totals[h], axis=-1, keepdims=True)
            out = (acc[h] / total).astype(jnp.bfloat16)
            own_ref[:, cols] = out[:rows]
            theirs_ref[:, cols] = out[rows:]


def guide_attention(heads, half, queries, gathered):
    rows, width = queries[0].shape
    keys = gathered.shape[0]
    block = min(KEY_BLOCK, keys)
    fixed = pl.BlockSpec((rows, width), lambda i, half: (0, 0))
    state = pltpu.VMEM((heads, 2 * rows, HDIM), jnp.float32)
    return pl.pallas_call(
        functools.partial(guide_attend, heads),
        out_shape=[jax.ShapeDtypeStruct((rows, width), jnp.bfloat16)] * 2,
        grid_spec=pltpu.PrefetchScalarGridSpec(
            num_scalar_prefetch=1,
            grid=(keys // block,),
            in_specs=[
                fixed,
                fixed,
                pl.BlockSpec((block, width), lambda i, half: (i, half[0])),
                pl.BlockSpec((block, width), lambda i, half: (i, 2 + half[0])),
            ],
            out_specs=[fixed, fixed],
            scratch_shapes=[state, state, state],
        ),
        compiler_params=pltpu.CompilerParams(dimension_semantics=("arbitrary",)),
        cost_estimate=pl.CostEstimate(
            flops=8 * rows * keys * width,
            transcendentals=2 * rows * keys * heads,
            bytes_accessed=4 * keys * width,
        ),
        name="guide_attention",
    )(half, *queries, gathered, gathered)


def head_out(summed, modulation, head_weight):
    centered = summed - jnp.mean(summed, axis=-1, keepdims=True)
    spread = jnp.mean(centered * centered, axis=-1, keepdims=True)
    normed = centered * lax.rsqrt(spread + 1e-06)
    shaped = (normed * (1.0 + modulation[1]) + modulation[0]).astype(jnp.bfloat16)
    return jnp.dot(shaped, head_weight, preferred_element_type=jnp.float32)


def per_device(
    members,
    latent,
    main_hidden,
    main_query,
    text_key,
    text_value,
    text_len,
    guide_hidden,
    guide_query,
    guide_key,
    guide_value,
    guide_out,
    main_head,
    guide_head,
    main_modulation,
    guide_modulation,
    guidance_scale,
    sigma_table,
    step_index,
):
    ring = members // 2
    me = lax.axis_index("seq")
    core, place = lax.rem(me, 2), lax.div(me, 2)
    partner = [(i, i ^ 1) for i in range(members)]
    ahead = [(i, (i + 2) % members) for i in range(members)]
    behind = [(i, (i - 2) % members) for i in range(members)]

    def half(x, which):
        width = x.shape[1] // 2
        return lax.dynamic_slice_in_dim(x, which * width, width, axis=1)

    def swap(x):
        return lax.ppermute(x, "seq", partner)

    def pair(k, v, which):
        return jnp.concatenate([half(k, which), half(v, which)], axis=1)

    guide_all = lax.all_gather(
        jnp.concatenate([guide_key, guide_value], axis=1), "seq", axis=0, tiled=True
    )
    mine = jnp.concatenate([half(text_key, core), half(text_value, core)], axis=1)
    theirs = jnp.concatenate([half(text_key, 1 - core), half(text_value, 1 - core)], axis=1)
    text_both = jnp.concatenate([mine, swap(theirs)], axis=0)
    main_queries = (half(main_query, core), swap(half(main_query, 1 - core)))
    guide_queries = (half(guide_query, core), swap(half(guide_query, 1 - core)))

    main_heads = main_head.shape[0] // HDIM // 2
    guide_heads = guide_out.shape[0] // HDIM // 2
    part = text_both.shape[1] // 2 // TEXT_CHAINS
    key_width = text_both.shape[1] // 2
    chains = [
        jnp.concatenate(
            [text_both[:, c * part : (c + 1) * part], text_both[:, key_width + c * part : key_width + (c + 1) * part]],
            axis=1,
        )
        for c in range(TEXT_CHAINS)
    ]
    up, down = list(chains), list(chains)
    held = {0: chains}
    order = [0]
    for step in range(1, ring // 2 + 1):
        both = step < ring - step
        up = [lax.ppermute(x, "seq", ahead) for x in up]
        held[step] = up
        order.append(step)
        if both:
            down = [lax.ppermute(x, "seq", behind) for x in down]
            held[ring - step] = down
            order.append(ring - step)

    rows = text_key.shape[0]
    inner = jnp.arange(2 * rows, dtype=jnp.int32)
    inner = jnp.where(inner < rows, core * rows + inner, (1 - core) * rows + inner - rows)
    owner = lax.rem(place - jnp.array(order, dtype=jnp.int32) + ring, ring)
    position = (owner[:, None] * (2 * rows) + inner[None, :]).reshape(1, -1)
    live = (position < text_len[0]).astype(jnp.float32)
    per_chain = main_heads // TEXT_CHAINS
    parts = [
        text_attention(c * per_chain, per_chain, main_queries, [held[j][c] for j in order], live)
        for c in range(TEXT_CHAINS)
    ]
    main_own = jnp.concatenate([p[0] for p in parts], axis=1)
    main_theirs = jnp.concatenate([p[1] for p in parts], axis=1)

    def whole(own, theirs):
        back = swap(theirs)
        return jnp.where(
            core == 0, jnp.concatenate([own, back], axis=1), jnp.concatenate([back, own], axis=1)
        )

    main_sum = main_hidden.astype(jnp.float32) + whole(main_own, main_theirs).astype(jnp.float32)
    main_velocity = head_out(main_sum, main_modulation, main_head)

    main_velocity = lax.optimization_barrier(main_velocity)

    guide_state = guide_attention(guide_heads, core.reshape(1), guide_queries, guide_all)
    projected = jnp.dot(whole(*guide_state), guide_out, preferred_element_type=jnp.float32)
    guide_sum = guide_hidden.astype(jnp.float32) + projected
    guide_velocity = head_out(guide_sum, guide_modulation, guide_head)
    velocity = guide_velocity + guidance_scale[0] * (main_velocity - guide_velocity)
    positions = jnp.arange(sigma_table.shape[0], dtype=jnp.int32)
    sigma_now = jnp.sum(jnp.where(positions == step_index[0], sigma_table, 0.0))
    sigma_next = jnp.sum(jnp.where(positions == step_index[0] + 1, sigma_table, 0.0))
    next_latent = latent + (sigma_next - sigma_now) * velocity
    return (velocity, next_latent)


def solution(mesh):
    placed = (
        P(("parts", "seq"), None),
        P(("parts", "seq"), None),
        P(("parts", "seq"), None),
        P(("parts", "seq"), None),
        P(("parts", "seq"), None),
        P("parts"),
        P(("parts", "seq"), None),
        P(("parts", "seq"), None),
        P(("parts", "seq"), None),
        P(("parts", "seq"), None),
        P(),
        P(),
        P(),
        P("parts", None),
        P("parts", None),
        P("parts"),
        P(),
        P("parts"),
    )
    return jax.shard_map(
        functools.partial(per_device, mesh.shape["seq"]),
        mesh=mesh,
        in_specs=placed,
        out_specs=(P(("parts", "seq"), None), P(("parts", "seq"), None)),
        check_vma=False,
    )
```
